256 devices in a mesh: section: 8 (over z_hi, core), batch: 8 (over x, z_lo), tile: 4 (over y).
Axes of the slice: x: 4, y: 4, z: 8 (z_hi: 4, z_lo: 2; z = z_hi * 2 + z_lo), core: 2. Of those that a mesh axis runs over, the one named last changes fastest.
Arguments:
- latents: bfloat16 [32, 4, 32, 1280], P('batch', 'tile'), parts along dimension 0, may hold values from -6 to 6
- prompt_tokens: bfloat16 [32, 77, 2048], P('batch'), parts along dimension 0, may hold values from -6 to 6
- fresh_noise: bfloat16 [1, 32, 4, 32, 1280], P(None, 'batch', 'tile'), parts along dimension 1, may hold values from -6 to 6
- timesteps: int32 [2], replicated, may hold values from 600 to 999
- entry_order: int32 [32], P('batch'), parts along dimension 0, may hold values from 0 to 3, each once
- timestep_weight: bfloat16 [8, 320, 1280], P('section'), may hold values from -0.3125 to 0.3125
- conv_kernel: float32 [8, 9, 1280], P('section'), may hold values from -1 to 1
- norm_gain: float32 [8, 1280], P('section'), may hold values from 0.25 to 1.75
- layer_norm_bias: float32 [8, 1280], P('section'), may hold values from -1.5 to 1.5
- qkv_weight: bfloat16 [8, 1280, 3, 1280], P('section', None, None, 'tile'), may hold values from -0.15625 to 0.15625
- prompt_weight: bfloat16 [8, 2048, 2, 1280], P('section', None, None, 'tile'), may hold values from -0.125 to 0.125
- out_weight: bfloat16 [8, 1280, 1280], P('section', 'tile'), may hold values from -0.15625 to 0.15625
Outputs:
- samples: bfloat16 [32, 4, 32, 1280], P('batch', 'tile', None, 'section'), parts along dimension 0
The draws below stay inside these ranges and needn't reach their ends.
There are 8 independent parts, one for each index of `batch`. The reference program is written for one: setup_inputs(seed, part) draws one part's arguments, and reference() takes and returns one part's arrays. A program takes and returns all parts, laid end to end along the dimension named above; an argument that names none is the same for every part. Nothing has to cross between parts.
All inputs are finite; a program needn't handle non-finite values.
Results may differ from the reference program's by a relative error of at most 0.019.
Values may be sent and summed in bfloat16 or wider, within the bound.
A program may use at most 64 MiB of HBM per device.

```python
import math
import jax
import jax.numpy as jnp
from jax import lax

WIDTH = 1280
HEADS = 20
TEXT_WIDTH = 2048
FREQS = 320
TEXT_TOKENS = 77
COLS = 32
ROWS = 4
MICRO = 4
STEPS = 2
N_SECTION = 8


def levels(stream_key, shape, split, low, largest):
    level = 1.0
    for axis_at, blocks in split:
        steps = jax.random.uniform(jax.random.fold_in(jax.random.fold_in(stream_key, 6), axis_at), (blocks,), jnp.float32, low / len(split), largest / len(split))
        level = level * jnp.repeat(jnp.exp(steps), shape[axis_at] // blocks).reshape((-1,) + (1,) * (len(shape) - 1 - axis_at))
    return level


def noise(key, shape, scale, most, shards=(), kind=jnp.bfloat16):
    drawn = jax.random.normal(key, shape, jnp.float32) * scale
    if len(shards) > 0:
        drawn = levels(key, shape, shards, -0.22, 0.18) * drawn
    return jnp.clip(drawn, min=-most, max=most).astype(kind)


def setup_inputs(seed: int = 0, part: int = 0) -> dict:
    seeds = jax.random.split(jax.random.key(seed), 13)
    own_keys = jax.random.split(jax.random.fold_in(seeds[12], part), 13)
    latents = noise(own_keys[0], (MICRO, ROWS, COLS, WIDTH), 1.0, 6.0, ((1, 4),))
    prompt_tokens = noise(own_keys[1], (MICRO, TEXT_TOKENS, TEXT_WIDTH), 1.0, 6.0)
    fresh_noise = noise(own_keys[2], (STEPS - 1, MICRO, ROWS, COLS, WIDTH), 1.0, 6.0, ((2, 4),))
    timesteps = jax.random.randint(seeds[3], (STEPS,), 600, 1000).astype(jnp.int32)
    entry_order = jax.random.permutation(own_keys[4], MICRO).astype(jnp.int32)
    timestep_weight = noise(seeds[5], (N_SECTION, FREQS, WIDTH), FREQS ** -0.5, 0.3125, ((0, 8),))
    conv_kernel = noise(seeds[6], (N_SECTION, 9, WIDTH), 0.2, 1.0, ((0, 8),), jnp.float32)
    norm_gain = jnp.clip(1.0 + 0.15 * jax.random.normal(seeds[7], (N_SECTION, WIDTH), jnp.float32), 0.25, 1.75)
    layer_norm_bias = noise(seeds[8], (N_SECTION, WIDTH), 0.3, 1.5, ((0, 8),), jnp.float32)
    qkv_weight = noise(seeds[9], (N_SECTION, WIDTH, 3, WIDTH), WIDTH ** -0.5, 0.15625, ((0, 8), (3, 4)))
    prompt_weight = noise(seeds[10], (N_SECTION, TEXT_WIDTH, 2, WIDTH), TEXT_WIDTH ** -0.5, 0.125, ((0, 8), (3, 4)))
    out_weight = noise(seeds[11], (N_SECTION, WIDTH, WIDTH), WIDTH ** -0.5, 0.15625, ((0, 8), (1, 4)))
    return dict(latents=latents, prompt_tokens=prompt_tokens, fresh_noise=fresh_noise, timesteps=timesteps, entry_order=entry_order, timestep_weight=timestep_weight, conv_kernel=conv_kernel, norm_gain=norm_gain, layer_norm_bias=layer_norm_bias, qkv_weight=qkv_weight, prompt_weight=prompt_weight, out_weight=out_weight)


def noise_plan():
    positions = jnp.arange(1000, dtype=jnp.float32)
    low_root = math.sqrt(0.00085)
    high_root = math.sqrt(0.012)
    roots = low_root + (high_root - low_root) * positions / 999.0
    return jnp.exp(jnp.cumsum(jnp.log(1.0 - roots * roots)))

def time_features(timesteps, half_count):
    exponents = jnp.arange(half_count, dtype=jnp.float32) / half_count
    freq_row = jnp.exp(-math.log(10000.0) * exponents)
    angles = timesteps.astype(jnp.float32)[:, None] * freq_row[None, :]
    return jnp.concatenate([jnp.cos(angles), jnp.sin(angles)], axis=1).astype(jnp.bfloat16)

def pick_scalar(alpha_table, position):
    hits = jnp.arange(alpha_table.shape[0], dtype=jnp.int32) == position
    return jnp.sum(jnp.where(hits, alpha_table, jnp.zeros_like(alpha_table)))

def mix_positions(rimmed, kernel_body):
    row_total = rimmed.shape[0] - 2
    col_total = rimmed.shape[1]
    framed = jnp.pad(rimmed.astype(jnp.float32), ((0, 0), (1, 1), (0, 0)))
    mixed = rimmed[1:-1].astype(jnp.float32)
    for offset_row in range(3):
        for offset_col in range(3):
            mixed = mixed + kernel_body[3 * offset_row + offset_col] * framed[offset_row:offset_row + row_total, offset_col:offset_col + col_total]
    return mixed

def layer_norm(values_in, scale_row, shift_row):
    centre = lax.optimization_barrier(jnp.mean(values_in, axis=-1, keepdims=True))
    spread = lax.optimization_barrier(jnp.mean(jnp.square(values_in - centre), axis=-1, keepdims=True))
    return (values_in - centre) * lax.rsqrt(spread + 1e-05) * scale_row + shift_row

def attention(queries, keys_all, values_all, head_count):
    query_count = queries.shape[0]
    key_count = keys_all.shape[0]
    head_width = queries.shape[1] // head_count
    query_heads = queries.astype(jnp.float32).reshape(query_count, head_count, head_width)
    key_heads = keys_all.astype(jnp.float32).reshape(key_count, head_count, head_width)
    value_heads = values_all.astype(jnp.float32).reshape(key_count, head_count, head_width)
    scores = jnp.einsum('qhd,khd->hqk', query_heads, key_heads) / math.sqrt(head_width)
    powers = jnp.exp(scores)
    soft_weights = (powers / lax.optimization_barrier(jnp.sum(powers, axis=-1, keepdims=True))).astype(jnp.bfloat16)
    attended = jnp.einsum('hqk,khd->qhd', soft_weights.astype(jnp.float32), value_heads)
    return attended.reshape(query_count, head_count * head_width).astype(jnp.bfloat16)

def run_section(current, temb_row, kernel_body, scale_row, shift_row, qkv_mat, prompt_mat, out_mat, prompt_row):
    rows_all, cols_all, width_all = current.shape
    lifted = (current.astype(jnp.float32) + temb_row).astype(jnp.bfloat16)
    rimmed = jnp.pad(lifted, ((1, 1), (0, 0), (0, 0)))
    mixed = mix_positions(rimmed, kernel_body).reshape(rows_all * cols_all, width_all)
    normed = layer_norm(mixed, scale_row, shift_row).astype(jnp.bfloat16)
    projected = jnp.einsum('tc,cjd->tjd', normed.astype(jnp.float32), qkv_mat.astype(jnp.float32)).astype(jnp.bfloat16)
    prompt_proj = jnp.einsum('tc,cjd->tjd', prompt_row.astype(jnp.float32), prompt_mat.astype(jnp.float32)).astype(jnp.bfloat16)
    keys_all = jnp.concatenate([projected[:, 1], prompt_proj[:, 0]], axis=0)
    values_all = jnp.concatenate([projected[:, 2], prompt_proj[:, 1]], axis=0)
    attended = attention(projected[:, 0], keys_all, values_all, HEADS)
    update = jnp.dot(attended, out_mat, preferred_element_type=jnp.float32)
    return (mixed + update).astype(jnp.bfloat16).reshape(rows_all, cols_all, width_all)

def reference(latents, prompt_tokens, fresh_noise, timesteps, entry_order, timestep_weight, conv_kernel, norm_gain, layer_norm_bias, qkv_weight, prompt_weight, out_weight):
    alpha_table = noise_plan()
    feature_rows = time_features(timesteps, timestep_weight.shape[1] // 2)
    timestep_embedding_all = jnp.einsum('zm,rmk->rzk', feature_rows.astype(jnp.float32), timestep_weight.astype(jnp.float32))
    results = jnp.zeros_like(latents)
    for slot_index in range(MICRO):
        latent_id = entry_order[slot_index].astype(jnp.int32)
        current = lax.dynamic_index_in_dim(latents, latent_id, 0, False)
        prompt_row = lax.dynamic_index_in_dim(prompt_tokens, latent_id, 0, False)
        for chain_level in range(STEPS):
            if chain_level > 0:
                alpha_bar = pick_scalar(alpha_table, timesteps[chain_level])
                current = (jnp.sqrt(alpha_bar) * current.astype(jnp.float32) + jnp.sqrt(1.0 - alpha_bar) * fresh_noise[chain_level - 1, slot_index].astype(jnp.float32)).astype(jnp.bfloat16)

            def section_step(state_now, section_inputs):
                temb_row, kernel_body, scale_row, shift_row, qkv_mat, prompt_mat, out_mat = section_inputs
                return (run_section(state_now, temb_row, kernel_body, scale_row, shift_row, qkv_mat, prompt_mat, out_mat, prompt_row), None)
            section_inputs = (timestep_embedding_all[:, chain_level], conv_kernel, norm_gain, layer_norm_bias, qkv_weight, prompt_weight, out_weight)
            scanned = lax.scan(section_step, current, section_inputs)
            current = scanned[0]
        results = results.at[latent_id].set(current)
    return results
```

```python
import functools
import math

import jax
import jax.numpy as jnp
from jax import lax
from jax.experimental import pallas as pl
from jax.experimental.pallas import tpu as pltpu
from jax.sharding import PartitionSpec as P

MESH = pl.DeviceIdType.MESH
F32 = jnp.float32
BF16 = jnp.bfloat16
WIDTH = 1280
HALF = 640
TOKENS = 128
TEXT = 77
TEXT_PAD = 80


def kernel(
    layers_z,
    order,
    steps,
    latents,
    noise,
    ptok,
    tweight,
    conv,
    gain,
    bias,
    wcat,
    wout,
    wprompt,
    out,
    wq,
    wo,
    ptok_v,
    wp_v,
    tw_v,
    pk_f,
    pk_s,
    pk_v,
    par,
    xin,
    nz,
    nsend,
    xc,
    mixed,
    normed,
    qkv,
    att,
    part_s,
    part_r,
    xs,
    fin,
    wr_sem,
    ws_sem,
    wrel_sem,
    own_l_sem,
    own_s_sem,
    own_r_sem,
    xa_s_sem,
    xa_r_sem,
    xa_l_sem,
    nz_s_sem,
    nz_r_sem,
    ld_sem,
    par_s_sem,
    par_r_sem,
    pk_s_sem,
    pk_r_sem,
    hop_s_sem,
    hop_r_sem,
    rel_s_sem,
    rel_r_sem,
    pt_s_sem,
    pt_r_sem,
    out_s_sem,
    out_r_sem,
):
    s = lax.axis_index("section")
    b = lax.axis_index("batch")
    t = lax.axis_index("tile")
    batches = lax.axis_size("batch")
    zh = s // 2
    c = s % 2
    oc = 1 - c
    p = (b // layers_z) % 2
    t_pair = t // 2
    t_low = t % 2
    is_own = c == t_pair
    b_up = lax.rem(b + layers_z, batches)
    b_down = lax.rem(b + batches - layers_z, batches)
    jd = 1 - t_low
    jf = t_low
    y_d = 2 * c + jd
    from_below = lax.rem(y_d + 1, 4) == t
    e_rel = jnp.where(from_below, 0, 1)
    t_rel = jnp.where(from_below, lax.rem(t + 1, 4), lax.rem(t + 3, 4))
    first = zh == 0
    last = zh == 3

    def remote(src, dst, ssem, rsem, **where):
        return pltpu.make_async_remote_copy(
            src_ref=src, dst_ref=dst, send_sem=ssem, recv_sem=rsem, device_id=where, device_id_type=MESH
        )

    def rows(start, size, unit):
        return pl.ds(pl.multiple_of(start, unit), size)

    barrier = pltpu.get_barrier_semaphore()

    def greet(n, _):
        s2 = n // 4
        t2 = n % 4

        @pl.when(jnp.logical_or(s2 != s, t2 != t))
        def _():
            pl.semaphore_signal(barrier, inc=1, device_id={"section": s2, "tile": t2}, device_id_type=MESH)

        return 0

    lax.fori_loop(0, 32, greet, 0)
    for b2 in (b_up, b_down):
        pl.semaphore_signal(barrier, inc=1, device_id={"batch": b2}, device_id_type=MESH)

    load_tok = pltpu.make_async_copy(ptok, ptok_v, ld_sem.at[0])
    load_wp = pltpu.make_async_copy(wprompt, wp_v, ld_sem.at[1])
    load_tw = pltpu.make_async_copy(tweight, tw_v, ld_sem.at[2])
    load_tw.start()
    load_tok.start()
    load_wp.start()

    pl.semaphore_wait(barrier, 33)

    def latent_copy(d, h):
        t2 = lax.rem(t + d, 4)
        return remote(
            latents.at[t2, :, pl.ds(HALF * h, HALF)],
            xin.at[0, h, rows(32 * t, 32, 32), :],
            xa_s_sem.at[d - 1, h],
            xa_r_sem.at[d - 1, h],
            tile=t2,
        )

    def latent_local(h):
        return pltpu.make_async_copy(
            latents.at[t, :, pl.ds(HALF * h, HALF)], xin.at[0, h, rows(32 * t, 32, 32), :], xa_l_sem.at[h]
        )

    @pl.when(first)
    def _():
        for d in (1, 3, 2):
            for h in range(2):
                latent_copy(d, h).start()
        for h in range(2):
            latent_local(h).start()

    def quarter(arr, q):
        return rows(320 * q, 320, 320) if arr == 0 else rows(80 * q, 80, 80)

    gathered = (wq, wo)
    sources = (wcat, wout)

    def direct_copy(arr, way, e):
        t2 = lax.rem(t + (1, 3)[way], 4)
        q = 2 * p + e
        return remote(
            sources[arr].at[quarter(arr, q), :],
            gathered[arr].at[c, t_low, quarter(arr, q), :],
            ws_sem.at[arr, way, e],
            wr_sem.at[arr, c, t_low, q],
            section=2 * zh + t_pair,
            tile=t2,
        )

    for arr in range(2):
        for e in range(2):
            for way in range(2):
                direct_copy(arr, way, (e + way) % 2).start()

    def own_local(arr):
        return pltpu.make_async_copy(sources[arr], gathered[arr].at[c, t_low], own_l_sem.at[arr])

    def own_remote(arr):
        return remote(
            sources[arr], gathered[arr].at[c, t_low], own_s_sem.at[arr], own_r_sem.at[arr], section=2 * zh + oc
        )

    def own_arrival(arr):
        return remote(
            sources[arr], gathered[arr].at[oc, t_low], own_s_sem.at[arr], own_r_sem.at[arr], section=2 * zh + oc
        )

    @pl.when(is_own)
    def _():
        for arr in range(2):
            own_local(arr).start()

    @pl.when(jnp.logical_not(is_own))
    def _():
        for arr in range(2):
            own_remote(arr).start()

    def noise_copy(d):
        t2 = lax.rem(t + d, 4)
        return remote(nsend.at[t2], nz.at[t], nz_s_sem.at[d - 1], nz_r_sem.at[d - 1], tile=t2)

    @pl.when(first)
    def _():
        for t2 in range(4):
            at = jnp.int32(0)
            for m in range(4):
                at = jnp.where(order[m] == t2, m, at)
            nsend[t2] = noise[at]
        for d in (1, 3, 2):
            noise_copy(d).start()
        nz[t] = nsend[t]

    par[c, 0:9, :] = conv[...]
    par[c, 9:10, :] = gain[...]
    par[c, 10:11, :] = bias[...]
    lane = lax.broadcasted_iota(jnp.int32, (16, 320), 1)
    row = lax.broadcasted_iota(jnp.int32, (16, 320), 0)
    spot = jnp.where(lane < 160, lane, lane - 160).astype(F32)
    freq = jnp.exp(-math.log(10000.0) * (spot / 160.0))
    moment = jnp.where(row == 0, steps[0].astype(F32), steps[1].astype(F32))
    angle = moment * freq
    feats = jnp.where(lane < 160, jnp.cos(angle), jnp.sin(angle)).astype(BF16)
    load_tw.wait()
    temb_all = jnp.dot(feats, tw_v[...], preferred_element_type=F32)
    par[c, 11:13, :] = temb_all[0:2]
    par_copy = remote(par.at[c], par.at[c], par_s_sem, par_r_sem, section=2 * zh + oc)
    par_copy.start()

    spots = (
        lax.broadcasted_iota(jnp.int32, (8, 128), 0) * 128 + lax.broadcasted_iota(jnp.int32, (8, 128), 1)
    )
    low_root = math.sqrt(0.00085)
    high_root = math.sqrt(0.012)
    roots = low_root + (high_root - low_root) * spots.astype(F32) / 999.0
    logs = jnp.where(spots <= steps[1], jnp.log(1.0 - roots * roots), 0.0)
    total = jnp.sum(jnp.sum(logs, axis=0, keepdims=True), axis=1, keepdims=True)
    alpha_bar = jnp.exp(total)
    keep = jnp.sqrt(alpha_bar)
    fresh = jnp.sqrt(1.0 - alpha_bar)

    pk_f[72:80, :] = jnp.zeros((8, HALF), F32)
    for i in range(2):
        for j in range(2):
            pk_v[i, j, TEXT_PAD:, :] = jnp.zeros((TOKENS - TEXT_PAD, HALF), BF16)
    load_tok.wait()
    load_wp.wait()

    def pk_copy(tt):
        return remote(
            pk_s.at[tt],
            pk_v.at[c, t_low, 0:TEXT_PAD, :],
            pk_s_sem.at[tt],
            pk_r_sem.at[c, t_low],
            section=2 * zh + t_pair,
            tile=tt,
        )

    def pk_is_self(tt):
        return jnp.logical_and(tt == t, is_own)

    def prompt_one(tt, _):
        pk_f[0:TEXT, :] = jnp.dot(ptok_v[tt], wp_v[...], preferred_element_type=F32)
        pk_s[tt] = pk_f[...].astype(BF16)

        @pl.when(jnp.logical_not(pk_is_self(tt)))
        def _():
            pk_copy(tt).start()

        @pl.when(pk_is_self(tt))
        def _():
            pk_v[c, t_low, 0:TEXT_PAD, :] = pk_s[tt]

        return 0

    lax.fori_loop(0, 4, prompt_one, 0)

    @pl.when(is_own)
    def _():
        for arr in range(2):
            own_local(arr).wait()
            own_arrival(arr).wait_recv()

    @pl.when(jnp.logical_not(is_own))
    def _():
        for arr in range(2):
            own_remote(arr).wait_send()

    def piece(arr, i, j, q):
        return gathered[arr].at[i, j, quarter(arr, q), :]

    def hand_on(arr, i, j, q, ssem, **where):
        return remote(piece(arr, i, j, q), piece(arr, i, j, q), ssem, wr_sem.at[arr, i, j, q], **where)

    def row_relay(arr, i):
        return hand_on(arr, i, jd, 2 * p + e_rel, wrel_sem.at[arr, i, 0], tile=t_rel)

    def side_relay(arr, i, j, e, slot):
        return hand_on(arr, i, j, 2 * p + e, wrel_sem.at[arr, i, slot], batch=(b_up, b_down)[e])

    def arrived(arr, i, j, q):
        hand_on(arr, i, j, q, wrel_sem.at[arr, i, 0], tile=t_rel).wait_recv()

    def relay(i, _):
        for arr in range(2):
            arrived(arr, i, jd, 2 * p + e_rel)
            row_relay(arr, i).start()
            arrived(arr, i, jd, 2 * p + 1 - e_rel)
            for e in range(2):
                side_relay(arr, i, jd, e, 1 + e).start()

        @pl.when(jnp.logical_not(is_own))
        def _():
            for arr in range(2):
                for e in range(2):
                    arrived(arr, i, jf, 2 * p + e)
                    side_relay(arr, i, jf, e, 3 + e).start()

        return 0

    lax.fori_loop(0, 2, relay, 0)

    par_arrival = remote(par.at[oc], par.at[oc], par_s_sem, par_r_sem, section=2 * zh + oc)
    par_arrival.wait_recv()

    def others(arr, i):
        for e in range(2):
            arrived(arr, i, jd, 2 * (1 - p) + e)

        @pl.when(jnp.logical_not(is_own))
        def _():
            for e in range(2):
                arrived(arr, i, jf, 2 * (1 - p) + e)

    def hop_copy(k, k_to):
        return remote(
            xs.at[k], xin.at[k_to, c], hop_s_sem.at[k], hop_r_sem.at[k_to], section=lax.rem(s + 2, 8)
        )

    def half_relay(k):
        return remote(xin.at[k, c], xin.at[k, c], rel_s_sem.at[k], rel_r_sem.at[k], section=2 * zh + oc)

    def half_arrival(k):
        return remote(xin.at[k, oc], xin.at[k, oc], rel_s_sem.at[k], rel_r_sem.at[k], section=2 * zh + oc)

    def part_copy(n, g):
        return remote(part_s.at[n, g], part_r.at[n, g], pt_s_sem.at[n, g], pt_r_sem.at[n, g], section=2 * zh + oc)

    def out_copy(q, t2):
        return remote(
            fin.at[q, rows(32 * t2, 32, 32), :],
            out.at[t],
            out_s_sem.at[q, t2],
            out_r_sem.at[t],
            section=4 * c + q,
            tile=t2,
        )

    column = lax.broadcasted_iota(jnp.int32, (TOKENS, 128), 0) % 32
    lane_row = lax.broadcasted_iota(jnp.int32, (1, 128), 1)
    low_f = jnp.where(lane_row < 64, 1.0, 0.0)
    lo = low_f.astype(BF16)
    hi = (1.0 - low_f).astype(BF16)
    is_low = lax.broadcasted_iota(jnp.int32, (TOKENS, 128), 1) < 64
    is_text = lax.broadcasted_iota(jnp.int32, (256, 256), 1) < TOKENS + TEXT
    scale = math.log2(math.e) / 8.0

    def stage(n, _):
        k = n // 2
        i = n % 2
        at_start = jnp.logical_and(first, k == 0)

        @pl.when(jnp.logical_and(i == 0, at_start))
        def _():
            for d in (1, 2, 3):
                for h in range(2):
                    latent_copy(d, h).wait_recv()
            for h in range(2):
                latent_local(h).wait()

        @pl.when(jnp.logical_and(i == 0, jnp.logical_not(at_start)))
        def _():
            hop_copy(k, k).wait_recv()
            half_relay(k).start()
            half_arrival(k).wait_recv()

        @pl.when(jnp.logical_and(i == 0, jnp.logical_and(first, k == 1)))
        def _():
            for d in (1, 2, 3):
                noise_copy(d).wait_recv()
            for h in range(2):
                for r in range(4):
                    old = xin[1, h, 32 * r : 32 * r + 32, :].astype(F32)
                    new = nz[r, :, HALF * h : HALF * h + HALF].astype(F32)
                    xc[h, 32 * r : 32 * r + 32, :] = (keep * old + fresh * new).astype(BF16)

        @pl.when(jnp.logical_and(i == 0, jnp.logical_not(jnp.logical_and(first, k == 1))))
        def _():
            xc[...] = xin[k]

        sums = jnp.zeros((TOKENS, 128), F32)
        for h in range(2):
            for l in range(5):
                ch = slice(HALF * h + 128 * l, HALF * h + 128 * l + 128)
                here = slice(128 * l, 128 * l + 128)
                temb = jnp.where(k == 0, par[i, 11:12, ch], par[i, 12:13, ch])
                lifted = (xc[h, :, here].astype(F32) + temb).astype(BF16).astype(F32)
                before = jnp.where(column == 0, 0.0, pltpu.roll(lifted, 1, 0))
                after = jnp.where(column == 31, 0.0, pltpu.roll(lifted, TOKENS - 1, 0))
                lines = []
                for a in range(3):
                    lines.append(
                        par[i, 3 * a : 3 * a + 1, ch] * before
                        + par[i, 3 * a + 1 : 3 * a + 2, ch] * lifted
                        + par[i, 3 * a + 2 : 3 * a + 3, ch] * after
                    )
                blank = jnp.zeros((32, 128), F32)
                above = jnp.concatenate([blank, lines[0][: TOKENS - 32]], axis=0)
                below = jnp.concatenate([lines[2][32:], blank], axis=0)
                got = lifted + above + lines[1] + below
                mixed[h, :, here] = got
                sums = sums + got
        centre = jnp.sum(sums, axis=1, keepdims=True) * (1.0 / WIDTH)
        squares = jnp.zeros((TOKENS, 128), F32)
        for h in range(2):
            for l in range(5):
                off = mixed[h, :, 128 * l : 128 * l + 128] - centre
                squares = squares + off * off
        spread = jnp.sum(squares, axis=1, keepdims=True) * (1.0 / WIDTH)
        inv = lax.rsqrt(spread + 1e-05)
        for h in range(2):
            for l in range(5):
                ch = slice(HALF * h + 128 * l, HALF * h + 128 * l + 128)
                off = mixed[h, :, 128 * l : 128 * l + 128] - centre
                normed[:, ch] = (off * inv * par[i, 9:10, ch] + par[i, 10:11, ch]).astype(BF16)

        @pl.when(k == 0)
        def _():
            others(0, i)

        for j in range(2):
            for m in range(4):
                cols = slice(256 * m, 256 * m + 256)
                qkv[j, :, cols] = jnp.dot(normed[...], wq[i, j, :, cols], preferred_element_type=F32).astype(BF16)

        @pl.when(k == 0)
        def _():
            for j in range(2):
                me = jnp.logical_and(i == c, 2 * c + j == t)

                @pl.when(jnp.logical_not(me))
                def _():
                    remote(
                        pk_s.at[0],
                        pk_v.at[i, j, 0:TEXT_PAD, :],
                        pk_s_sem.at[0],
                        pk_r_sem.at[i, j],
                        section=2 * zh + oc,
                    ).wait_recv()

        def block(j, m):
            return qkv[j, :, 128 * m : 128 * m + 128]

        def text(j, m):
            return pk_v[i, j, :, 128 * m : 128 * m + 128]

        heads = []
        for j in range(2):
            heads.append((block(j, 0), block(j, 3), block(j, 5), text(j, 0), text(j, 2), False))
            heads.append((block(j, 1), block(j, 4), block(j, 6), text(j, 1), text(j, 3), False))
        heads.append(
            (
                block(0, 2) * lo + block(1, 2) * hi,
                block(0, 7) + block(1, 7),
                block(1, 2) * lo + block(0, 2) * hi,
                text(0, 4) * lo + text(1, 4) * hi,
                text(1, 4) * lo + text(0, 4) * hi,
                True,
            )
        )
        for at, (q_pair, k_self, v_self, k_text, v_text, crossed) in enumerate(heads):
            lhs = jnp.concatenate([q_pair * lo, q_pair * hi], axis=0)
            keys = jnp.concatenate([k_self, k_text], axis=0)
            vals = jnp.concatenate([v_self, v_text], axis=0)
            scores = lax.dot_general(lhs, keys, (((1,), (1,)), ((), ())), preferred_element_type=F32)
            powers = jnp.where(is_text, jnp.exp2(scores * scale), 0.0)
            inverse = 1.0 / jnp.sum(powers, axis=1, keepdims=True)
            weights = (powers * inverse).astype(BF16)
            got = jnp.dot(weights, vals, preferred_element_type=F32)
            top, bottom = got[:TOKENS], got[TOKENS:]
            pair = jnp.where(is_low, bottom, top) if crossed else jnp.where(is_low, top, bottom)
            att[:, 128 * at : 128 * at + 128] = pair.astype(BF16)

        @pl.when(k == 0)
        def _():
            others(1, i)

        def product(g):
            cols = rows(HALF * g, HALF, 128)
            mat = jnp.concatenate(
                [
                    wo[i, 0, 0:256, cols],
                    wo[i, 1, 0:256, cols],
                    wo[i, 1, 256:320, cols],
                    wo[i, 0, 256:320, cols],
                ],
                axis=0,
            )
            return jnp.dot(att[...], mat, preferred_element_type=F32).astype(BF16)

        part_s[n, oc] = product(oc)
        part_copy(n, oc).start()
        part_s[n, c] = product(c)

        @pl.when(i == 0)
        def _():
            part_copy(n, c).start()

        def added(g):
            update = part_s[n, g].astype(F32) + part_r[n, g].astype(F32)
            return (mixed[g] + update).astype(BF16)

        part_copy(n, c).wait_recv()
        mine = added(c)

        @pl.when(i == 0)
        def _():
            xc[c] = mine
            part_copy(n, oc).wait_recv()
            xc[oc] = added(oc)

        at_end = jnp.logical_and(last, k == 1)

        @pl.when(jnp.logical_and(i == 1, jnp.logical_not(at_end)))
        def _():
            xs[k] = mine
            hop_copy(k, jnp.where(last, 1, k)).start()

        @pl.when(jnp.logical_and(i == 1, at_end))
        def _():
            for q in range(4):
                fin[q] = mine[:, 160 * q : 160 * q + 160]
            for q in range(4):
                for t2 in range(4):
                    own = jnp.logical_and(s == 4 * c + q, t == t2)

                    @pl.when(jnp.logical_not(own))
                    def _():
                        out_copy(q, t2).start()

                    @pl.when(own)
                    def _():
                        out[t] = fin[q, 32 * t2 : 32 * t2 + 32, :]

        return 0

    lax.fori_loop(0, 4, stage, 0)

    for t2 in range(4):
        own = jnp.logical_and(s == 7, t == t2)

        @pl.when(jnp.logical_not(own))
        def _():
            remote(
                fin.at[0, 0:32, :], out.at[t2], out_s_sem.at[0, 0], out_r_sem.at[t2], section=2 * zh + oc
            ).wait_recv()

    @pl.when(last)
    def _():
        for q in range(4):
            for t2 in range(4):
                own = jnp.logical_and(s == 4 * c + q, t == t2)

                @pl.when(jnp.logical_not(own))
                def _():
                    out_copy(q, t2).wait_send()

    @pl.when(first)
    def _():
        for d in (1, 2, 3):
            for h in range(2):
                latent_copy(d, h).wait_send()
            noise_copy(d).wait_send()

    for arr in range(2):
        for way in range(2):
            for e in range(2):
                direct_copy(arr, way, e).wait_send()
    par_copy.wait_send()
    for tt in range(4):

        @pl.when(jnp.logical_not(pk_is_self(tt)))
        def _():
            pk_copy(tt).wait_send()

    for i in range(2):
        for arr in range(2):
            row_relay(arr, i).wait_send()
            for e in range(2):
                side_relay(arr, i, jd, e, 1 + e).wait_send()

        @pl.when(jnp.logical_not(is_own))
        def _():
            for arr in range(2):
                for e in range(2):
                    side_relay(arr, i, jf, e, 3 + e).wait_send()

    for n in range(4):
        part_copy(n, oc).wait_send()
        if n % 2 == 0:
            part_copy(n, c).wait_send()
    for k in range(2):

        @pl.when(jnp.logical_not(jnp.logical_and(first, k == 0)))
        def _():
            half_relay(k).wait_send()

        @pl.when(jnp.logical_not(jnp.logical_and(last, k == 1)))
        def _():
            hop_copy(k, jnp.where(last, 1, k)).wait_send()


def arranged(low, parts, first_odd, second_odd):
    odd = jnp.where(low == 0, jnp.concatenate([first_odd, second_odd], 1), jnp.concatenate([second_odd, first_odd], 1))
    return jnp.concatenate([*parts, odd], axis=1)


def per_device(
    layers_z,
    latents,
    prompt_tokens,
    fresh_noise,
    timesteps,
    entry_order,
    timestep_weight,
    conv_kernel,
    norm_gain,
    layer_norm_bias,
    qkv_weight,
    prompt_weight,
    out_weight,
):
    low = lax.axis_index("tile") % 2
    q, k, v = (qkv_weight[0, :, m] for m in range(3))
    blank = jnp.zeros((q.shape[0], 64), BF16)
    odd = jnp.where(low == 0, jnp.concatenate([q[:, 256:], v[:, 256:]], 1), jnp.concatenate([v[:, 256:], q[:, 256:]], 1))
    rest = jnp.where(low == 0, jnp.concatenate([k[:, 256:], blank], 1), jnp.concatenate([blank, k[:, 256:]], 1))
    wcat = jnp.concatenate([q[:, :256], odd, k[:, :256], v[:, :256], rest], axis=1)
    pk, pv = prompt_weight[0, :, 0], prompt_weight[0, :, 1]
    wprompt = arranged(low, [pk[:, :256], pv[:, :256]], pk[:, 256:], pv[:, 256:])

    vmem = pl.BlockSpec(memory_space=pltpu.VMEM)
    smem = pl.BlockSpec(memory_space=pltpu.SMEM)
    held = pl.BlockSpec(memory_space=pl.ANY)
    dma = pltpu.SemaphoreType.DMA
    micro, _, cols, width = latents.shape
    return pl.pallas_call(
        functools.partial(kernel, layers_z),
        out_shape=jax.ShapeDtypeStruct((micro, cols, width // 8), BF16),
        in_specs=[smem, smem, held, vmem, held, held, vmem, vmem, vmem, held, held, held],
        out_specs=vmem,
        scratch_shapes=[
            pltpu.VMEM((2, 2, WIDTH, 1024), BF16),
            pltpu.VMEM((2, 2, 320, WIDTH), BF16),
            pltpu.VMEM((4, TEXT, 2048), BF16),
            pltpu.VMEM((2048, HALF), BF16),
            pltpu.VMEM((320, WIDTH), BF16),
            pltpu.VMEM((TEXT_PAD, HALF), F32),
            pltpu.VMEM((4, TEXT_PAD, HALF), BF16),
            pltpu.VMEM((2, 2, TOKENS, HALF), BF16),
            pltpu.VMEM((2, 16, WIDTH), F32),
            pltpu.VMEM((2, 2, TOKENS, HALF), BF16),
            pltpu.VMEM((4, 32, WIDTH), BF16),
            pltpu.VMEM((4, 32, WIDTH), BF16),
            pltpu.VMEM((2, TOKENS, HALF), BF16),
            pltpu.VMEM((2, TOKENS, HALF), F32),
            pltpu.VMEM((TOKENS, WIDTH), BF16),
            pltpu.VMEM((2, TOKENS, 1024), BF16),
            pltpu.VMEM((TOKENS, HALF), BF16),
            pltpu.VMEM((4, 2, TOKENS, HALF), BF16),
            pltpu.VMEM((4, 2, TOKENS, HALF), BF16),
            pltpu.VMEM((2, TOKENS, HALF), BF16),
            pltpu.VMEM((4, TOKENS, 160), BF16),
            dma((2, 2, 2, 4)),
            dma((2, 2, 2)),
            dma((2, 2, 5)),
            dma((2,)),
            dma((2,)),
            dma((2,)),
            dma((3, 2)),
            dma((3, 2)),
            dma((2,)),
            dma((3,)),
            dma((3,)),
            dma((3,)),
            dma,
            dma,
            dma((4,)),
            dma((2, 2)),
            dma((2,)),
            dma((2,)),
            dma((2,)),
            dma((2,)),
            dma((4, 2)),
            dma((4, 2)),
            dma((4, 4)),
            dma((4,)),
        ],
        compiler_params=pltpu.CompilerParams(collective_id=0, has_side_effects=True),
    )(
        entry_order,
        timesteps,
        latents[:, 0],
        fresh_noise[0, :, 0],
        prompt_tokens,
        timestep_weight[0],
        conv_kernel[0],
        norm_gain,
        layer_norm_bias,
        wcat,
        out_weight[0],
        wprompt,
    )[:, None]


def solution(mesh):
    layers_z = 2 if mesh.shape["batch"] >= 4 else 1
    placed = (
        P("batch", "tile", None, None),
        P("batch", None, None),
        P(None, "batch", "tile", None, None),
        P(),
        P("batch"),
        P("section", None, None),
        P("section", None, None),
        P("section", None),
        P("section", None),
        P("section", None, None, "tile"),
        P("section", None, None, "tile"),
        P("section", "tile", None),
    )
    return jax.shard_map(
        functools.partial(per_device, layers_z),
        mesh=mesh,
        in_specs=placed,
        out_specs=P("batch", "tile", None, "section"),
        check_vma=False,
    )
```
